32 devices in a mesh: groups: 2 (over y), kvb: 4 (over z), tp: 4 (over x, core).
Axes of the slice: x: 2, y: 2, z: 4, core: 2. Of those that a mesh axis runs over, the one named last changes fastest.
Arguments:
- residual: bfloat16 [32, 8192], P(('groups', 'kvb')), parts along dimension 0, may hold values from -3 to 3
- queries: bfloat16 [32, 8192], P(('groups', 'kvb'), 'tp'), parts along dimension 0, may hold values from -60 to 60
- new_kv: bfloat16 [32, 2048], P(('groups', 'kvb')), parts along dimension 0, may hold values from -6 to 6
- kv_cache: bfloat16 [2048, 16, 2048], P(('groups', 'kvb', 'tp')), parts along dimension 0, may hold values from -6 to 6
- lengths: int32 [32], P('groups'), parts along dimension 0, may hold values from 1 to 2048, as said below
- slot_seq: int32 [2048], P(('groups', 'kvb', 'tp')), parts along dimension 0, may hold values from 0 to 15, as said below
- slot_block: int32 [2048], P(('groups', 'kvb', 'tp')), parts along dimension 0, may hold values from 0 to 127, as said below
- block_counts: int32 [32], P(('groups', 'kvb', 'tp')), parts along dimension 0, may hold values from 16 to 64, as said below
- out_weight: bfloat16 [8192, 8192], P('tp'), may hold values from -0.5 to 0.5
- norm_gain: bfloat16 [8192], P('tp'), may hold values from 0.099609375 to 1.8984375
Outputs:
- stream: bfloat16 [32, 8192], P(('groups', 'kvb'), 'tp'), parts along dimension 0
- normed: bfloat16 [32, 8192], P(('groups', 'kvb'), 'tp'), parts along dimension 0
The draws below stay inside these ranges and needn't reach their ends.
There are 2 independent parts, one for each index of `groups`. The reference program is written for one: setup_inputs(seed, part) draws one part's arguments, and reference() takes and returns one part's arrays. A program takes and returns all parts, laid end to end along the dimension named above; an argument that names none is the same for every part. Nothing has to cross between parts.
Inputs may be any that keep to these rules, and one draw needn't show every extreme that they name: `block_counts`: slots below a device's count hold cache blocks, those at or beyond it none; at least one device's count is 64. `slot_seq`: each pair of a sequence s and a block b below ceil(lengths[s] / 16) sits in exactly one live slot of the group. `slot_block`: some sequence has exactly 128 blocks; none has more. `lengths`: some sequence has exactly 16 * (128) tokens.
All inputs are finite; a program needn't handle non-finite values.
Results may differ from the reference program's by a relative error of at most 0.006.
Values may be sent and summed in bfloat16 or wider, within the bound.
A program may use at most 64 MiB of HBM per device.

```python
import jax
import jax.numpy as jnp
from jax import lax

D = 8192
QH = 64
KVH = 8
HD = 128
BLK = 16
POOL = 64
GROUP = 16
SEQS = 16
SLOTS = 1024


def layout(key):
    base = jax.random.fold_in(key, 7)
    streams = jax.random.split(base, 8)
    floor_count = max(POOL // 4, 1)
    divider = jax.random.randint(streams[0], (GROUP,), 1, 5)
    jitter = jax.random.randint(streams[1], (GROUP,), 0, 4)
    counts = jnp.maximum(POOL // divider - jitter, floor_count)
    fullest = jax.random.randint(streams[2], (), 0, GROUP)
    counts = jnp.where(jnp.arange(GROUP) == fullest, POOL, counts).astype(jnp.int32)
    used = (jnp.arange(POOL)[None, :] < counts[:, None]).reshape(-1)
    priority = jax.random.permutation(streams[3], SLOTS).astype(jnp.int32)
    priority = jnp.where(used, priority, priority + SLOTS)
    order = jnp.argsort(priority)
    rank = jnp.argsort(order).astype(jnp.int32)
    total_used = jnp.sum(counts).astype(jnp.int32)
    most_blocks = SLOTS // 8
    longest = jax.random.randint(streams[7], (), 0, SEQS)
    seq_ids = jnp.arange(SEQS, dtype=jnp.int32)
    is_long = seq_ids == longest
    remaining = total_used - most_blocks
    seq_weight = jnp.where(is_long, 0, jax.random.randint(streams[4], (SEQS,), 1, 64)).astype(jnp.int32)
    cumulative = jnp.cumsum(seq_weight).astype(jnp.int32)
    share_ends = (remaining - (SEQS - 1)) * cumulative // cumulative[-1]
    share_starts = jnp.concatenate([jnp.zeros((1,), jnp.int32), share_ends[:-1]])
    proposed = jnp.where(is_long, 0, share_ends - share_starts + 1)
    capped = jnp.minimum(proposed, most_blocks)
    deficit = remaining - jnp.sum(capped)
    headroom = jnp.where(is_long, 0, most_blocks - capped)
    before = jnp.cumsum(headroom) - headroom
    extra = jnp.clip(deficit - before, 0, headroom)
    blocks = jnp.where(is_long, most_blocks, capped + extra).astype(jnp.int32)
    ends = jnp.cumsum(blocks).astype(jnp.int32)
    starts = (ends - blocks).astype(jnp.int32)
    owner = jnp.sum((rank[:, None] >= ends[None, :]).astype(jnp.int32), axis=1)
    owner = jnp.minimum(owner, SEQS - 1)
    start_of = jnp.take(starts, owner)
    filler = jax.random.randint(streams[5], (SLOTS,), 0, SEQS)
    seq_table = jnp.where(used, owner, filler).astype(jnp.int32)
    block_table = jnp.where(used, rank - start_of, 0).astype(jnp.int32)
    dropped = jnp.where(is_long, 0, jax.random.randint(streams[6], (SEQS,), 0, BLK))
    seq_lengths = (BLK * blocks - dropped).astype(jnp.int32)
    return (seq_lengths, seq_table, block_table, counts)


def draw_lengths(key, part):
    return layout(key)[0]


def draw_slot_seq(key, part):
    return layout(key)[1]


def draw_slot_block(key, part):
    return layout(key)[2]


def draw_block_counts(key, part):
    return layout(key)[3]


def draw_kv_cache(key, part):
    cache = jax.random.normal(jax.random.fold_in(key, 29), (SLOTS, BLK, 2 * KVH * HD), jnp.float32)
    cache = jnp.clip(cache, -6.0, 6.0)
    return cache.astype(jnp.bfloat16)


def draw_queries(key, part):
    values = jax.random.normal(jax.random.fold_in(key, 41), (SEQS, QH * HD), jnp.float32)
    values = jnp.clip(values, -6.0, 6.0)
    return values.astype(jnp.bfloat16)


def levels(key, extent, shards, least, high):
    def one(dim, blocks):
        steps = jax.random.uniform(jax.random.fold_in(jax.random.fold_in(key, 6), dim), (blocks,), jnp.float32, least / len(shards), high / len(shards))
        return jnp.repeat(jnp.exp(steps), extent[dim] // blocks).reshape((-1,) + (1,) * (len(extent) - dim - 1))

    loudness = one(*shards[0])
    for cut in shards[1:]:
        loudness = loudness * one(*cut)
    return loudness


def noise(own_key, extent, scale, reach, shards=(), kind=jnp.bfloat16):
    drawn = jax.random.normal(own_key, extent, jnp.float32) * scale
    if len(shards) > 0:
        drawn = levels(own_key, extent, shards, -0.22, 0.18) * drawn
    return jnp.clip(drawn, min=-reach, max=reach).astype(kind)


def setup_inputs(seed: int = 0, part: int = 0) -> dict:
    streams_of = jax.random.split(jax.random.key(seed), 11)
    own_keys = jax.random.split(jax.random.fold_in(streams_of[10], part), 11)
    residual = noise(own_keys[0], (SEQS, D), 0.5, 3.0, ((0, 4),))
    queries = draw_queries(jax.random.fold_in(jax.random.fold_in(streams_of[10], part), 71), part)
    new_kv = noise(own_keys[2], (SEQS, 2 * KVH * HD), 1.0, 6.0, ((0, 4),))
    kv_cache = draw_kv_cache(jax.random.fold_in(jax.random.fold_in(streams_of[10], part), 71), part)
    lengths = draw_lengths(jax.random.fold_in(jax.random.fold_in(streams_of[10], part), 71), part)
    slot_seq = draw_slot_seq(jax.random.fold_in(jax.random.fold_in(streams_of[10], part), 71), part)
    slot_block = draw_slot_block(jax.random.fold_in(jax.random.fold_in(streams_of[10], part), 71), part)
    block_counts = draw_block_counts(jax.random.fold_in(jax.random.fold_in(streams_of[10], part), 71), part)
    out_weight = noise(streams_of[8], (QH * HD, D), HD ** -0.5, 0.5, ((0, 4),))
    norm_gain = jnp.clip(1.0 + 0.18 * jax.random.normal(streams_of[9], (D,), jnp.float32), 0.099609375, 1.8984375).astype(jnp.bfloat16)
    return dict(residual=residual, queries=queries, new_kv=new_kv, kv_cache=kv_cache, lengths=lengths, slot_seq=slot_seq, slot_block=slot_block, block_counts=block_counts, out_weight=out_weight, norm_gain=norm_gain)


NEGATIVE = -1e+30
EPSILON = 1e-06

def pool_partial(grouped, cache_pool, seq_pool, block_pool, live_count, lengths):
    pool_size = cache_pool.shape[0]
    key_rows = cache_pool[:, :, :KVH * HD].reshape(pool_size * BLK, KVH, HD).astype(jnp.float32)
    value_rows = cache_pool[:, :, KVH * HD:].reshape(pool_size * BLK, KVH, HD).astype(jnp.float32)
    token_seq = jnp.repeat(seq_pool, BLK)
    position = (block_pool[:, None] * BLK + jnp.arange(BLK, dtype=jnp.int32)[None, :]).reshape(-1)
    slot_live = jnp.repeat(jnp.arange(pool_size, dtype=jnp.int32) < live_count, BLK)
    member = token_seq[None, :] == jnp.arange(SEQS, dtype=jnp.int32)[:, None]
    length_of = lax.optimization_barrier(jnp.sum(jnp.where(member, lengths[:, None], 0), axis=0))
    live = member & (position < length_of)[None, :] & slot_live[None, :]
    mask = live[:, None, None, :]
    scores = jnp.einsum('sgqd,ngd->sgqn', grouped.astype(jnp.float32), key_rows) * HD ** (-0.5)
    peak_now = lax.optimization_barrier(jnp.max(jnp.where(mask, scores, NEGATIVE), axis=-1))
    weights = jnp.where(mask, jnp.exp(scores - peak_now[..., None]), 0.0)
    weight_sum = lax.optimization_barrier(jnp.sum(weights, axis=-1))
    rounded = weights.astype(jnp.bfloat16).astype(jnp.float32)
    partial_rows = jnp.einsum('sgqn,ngd->sgqd', rounded, value_rows)
    return (peak_now, weight_sum, partial_rows)

def reference(residual, queries, new_kv, kv_cache, lengths, slot_seq, slot_block, block_counts, out_weight, norm_gain):
    grouped = queries.reshape(SEQS, KVH, QH // KVH, HD)
    cache_groups = kv_cache.reshape(GROUP, POOL, BLK, 2 * KVH * HD)
    seq_groups = slot_seq.reshape(GROUP, POOL)
    block_groups = slot_block.reshape(GROUP, POOL)

    def one_pool(pieces):
        return pool_partial(grouped, pieces[0], pieces[1], pieces[2], pieces[3], lengths)
    peaks, sums, partials = lax.map(one_pool, (cache_groups, seq_groups, block_groups, block_counts))
    new_keys = new_kv[:, :KVH * HD].reshape(SEQS, KVH, HD).astype(jnp.float32)
    new_values = new_kv[:, KVH * HD:].reshape(SEQS, KVH, HD).astype(jnp.float32)
    fresh = jnp.einsum('sgqd,sgd->sgq', grouped.astype(jnp.float32), new_keys) * HD ** (-0.5)
    overall = jnp.maximum(lax.optimization_barrier(jnp.max(peaks, axis=0)), fresh)
    scaling = jnp.exp(peaks - overall[None])
    fresh_weight = jnp.exp(fresh - overall)
    denominator = lax.optimization_barrier(jnp.sum(scaling * sums, axis=0)) + fresh_weight
    numerator = lax.optimization_barrier(jnp.sum(scaling[..., None] * partials, axis=0)) + fresh_weight[..., None] * new_values[:, :, None, :]
    attended = (numerator / denominator[..., None]).reshape(SEQS, QH * HD).astype(jnp.bfloat16)
    projected = jnp.dot(attended, out_weight, preferred_element_type=jnp.float32)
    stream = (residual.astype(jnp.float32) + projected).astype(jnp.bfloat16)
    stream_wide = lax.optimization_barrier(stream).astype(jnp.float32)
    mean_square = lax.optimization_barrier(jnp.mean(stream_wide * stream_wide, axis=1, keepdims=True))
    normed = (stream_wide * lax.rsqrt(mean_square + EPSILON) * norm_gain.astype(jnp.float32)).astype(jnp.bfloat16)
    return (stream, normed)
```

```python
import math

import jax
import jax.numpy as jnp
from jax import lax
from jax.experimental import pallas as pl
from jax.experimental.pallas import tpu as pltpu
from jax.sharding import PartitionSpec as P

QH = 64
KVH = 8
HD = 128
BLK = 16
GROUP_HEADS = QH // KVH

NEGATIVE = -1e30
EPSILON = 1e-06
LANES = 128
TOKEN_LOG2 = math.log2(math.e) * HD ** (-0.5)
MESH = pl.DeviceIdType.MESH


def kernel(
    nz,
    nt,
    seq_rep,
    local_heads,
    lengths_ref,
    counts_ref,
    slot_seq_ref,
    slot_block_ref,
    residual_ref,
    queries_ref,
    new_kv_ref,
    gain_ref,
    cache_ref,
    weight_ref,
    stream_ref,
    normed_ref,
    cache_buf,
    weight_buf,
    bias_buf,
    row_buf,
    new_buf,
    q_all,
    part_tp,
    stat_tp,
    part_send,
    stat_send,
    z_send,
    z_stat_send,
    z_part,
    z_stat,
    lhs_buf,
    proj_send,
    proj_recv,
    ss_send,
    ss_recv,
    cache_sem,
    weight_sem,
    qz_send,
    qz_recv,
    qt_send,
    qt_recv,
    pt_send,
    pt_recv,
    st_send,
    st_recv,
    zp_send,
    zp_recv,
    zs_send,
    zs_recv,
    rs_send,
    rs_recv,
    sq_send,
    sq_recv,
):
    z = lax.axis_index("kvb")
    t = lax.axis_index("tp")
    kv_local = max(1, local_heads // GROUP_HEADS)
    per_kv = local_heads // kv_local
    sub = per_kv * seq_rep
    rows = nz * sub
    tokens = cache_buf.shape[0]
    slots = slot_seq_ref.shape[1]
    width = gain_ref.shape[1]
    fast = 2 if nt % 2 == 0 else 1
    slow = nt // fast

    def tp_to(j):
        return lax.rem(t // fast + j // fast, slow) * fast + lax.rem(t % fast + j % fast, fast)

    def tp_from(j):
        back = (slow - j // fast) % slow
        back_fast = (fast - j % fast) % fast
        return lax.rem(t // fast + back, slow) * fast + lax.rem(t % fast + back_fast, fast)

    def z_to(a):
        return lax.rem(z + a, nz)

    def z_back(a):
        return lax.rem(z + (nz - a), nz)

    far_first = sorted(range(1, nt), key=lambda j: (j < fast, j))

    cache_copy = pltpu.make_async_copy(cache_ref, cache_buf, cache_sem)
    cache_copy.start()
    weight_copies = {}
    for j in far_first + [0]:
        columns = pl.ds(pl.multiple_of(tp_to(j) * width, LANES), width)
        weight_copies[j] = pltpu.make_async_copy(
            weight_ref.at[:, columns], weight_buf.at[j], weight_sem.at[j]
        )
        weight_copies[j].start()

    barrier = pltpu.get_barrier_semaphore()
    for a in range(1, nz):
        pl.semaphore_signal(barrier, inc=1, device_id={"kvb": z_to(a)}, device_id_type=MESH)
    for j in range(1, nt):
        pl.semaphore_signal(barrier, inc=1, device_id={"tp": tp_to(j)}, device_id_type=MESH)

    wide_q = queries_ref[...].astype(jnp.float32)
    for k in range(kv_local):
        for q in range(per_kv):
            head = k * per_kv + q
            row_buf[k, q * seq_rep : (q + 1) * seq_rep, :] = wide_q[:, head * HD : (head + 1) * HD]
    for k in range(kv_local):
        q_all[0, 0, k] = row_buf[k].astype(jnp.bfloat16)
    pl.semaphore_wait(barrier, nz - 1 + nt - 1)

    pending = []

    def remote(src, dst, send, recv, target):
        copy = pltpu.make_async_remote_copy(
            src_ref=src,
            dst_ref=dst,
            send_sem=send,
            recv_sem=recv,
            device_id=target,
            device_id_type=MESH,
        )
        copy.start()
        pending.append(copy)
        return copy

    z_order = sorted(range(1, nz), key=lambda a: min(a, nz - a))
    q_from_z = {}
    for a in reversed(z_order):
        q_from_z[a] = remote(
            q_all.at[0, 0], q_all.at[0, a], qz_send.at[a], qz_recv.at[a], {"kvb": z_to(a)}
        )
    q_from_tp = {}

    def forward(a):
        for j in far_first:
            q_from_tp[a, j] = remote(
                q_all.at[0, a],
                q_all.at[j, a],
                qt_send.at[a, j],
                qt_recv.at[a, j],
                {"tp": tp_to(j)},
            )

    forward(0)

    row_id = lax.broadcasted_iota(jnp.int32, (rows, slots), 0)
    slot_id = lax.broadcasted_iota(jnp.int32, (rows, slots), 1)
    row_seq = lax.rem(z + nz - row_id // sub, nz) * seq_rep + lax.rem(row_id, seq_rep)
    row_len = jnp.zeros((rows, slots), jnp.int32)
    for s in range(nz * seq_rep):
        row_len = jnp.where(row_seq == s, lengths_ref[s], row_len)
    held = (row_seq == slot_seq_ref[...]) & (slot_id < counts_ref[0])
    limit = jnp.where(held, jnp.clip(row_len - BLK * slot_block_ref[...], 0, BLK), 0)
    token_slot = lax.broadcasted_iota(jnp.int32, (slots, tokens), 1) // BLK
    spread = (token_slot == lax.broadcasted_iota(jnp.int32, (slots, tokens), 0)).astype(jnp.float32)
    reach = jnp.dot(
        limit.astype(jnp.float32).astype(jnp.bfloat16),
        spread.astype(jnp.bfloat16),
        preferred_element_type=jnp.float32,
    )
    offset = lax.rem(lax.broadcasted_iota(jnp.int32, (rows, tokens), 1), BLK).astype(jnp.float32)
    bias_buf[...] = jnp.where(offset < reach, 0.0, NEGATIVE)

    own_kv = t * local_heads // GROUP_HEADS
    fresh = []
    for k in range(kv_local):
        for part in range(2):
            at = pl.multiple_of((part * KVH + own_kv + k) * HD, LANES)
            piece = new_kv_ref[:, pl.ds(at, HD)].astype(jnp.float32)
            for q in range(per_kv):
                new_buf[k, part, q * seq_rep : (q + 1) * seq_rep, :] = piece
        fresh.append(jnp.sum(row_buf[k] * new_buf[k, 0], axis=1, keepdims=True) * TOKEN_LOG2)
    lhs_buf[...] = jnp.zeros_like(lhs_buf)

    for a in z_order:
        q_from_z[a].wait_recv()
        forward(a)

    cache_copy.wait()
    lane = lax.broadcasted_iota(jnp.int32, (rows, LANES), 1)
    parts, stats = {}, {}
    for j in range(nt):
        if j > 0:
            for a in range(nz):
                q_from_tp[a, j].wait_recv()
        first_kv = tp_from(j) * local_heads // GROUP_HEADS
        for k in range(kv_local):
            key_at = pl.multiple_of((first_kv + k) * HD, LANES)
            value_at = pl.multiple_of((KVH + first_kv + k) * HD, LANES)
            q_rows = q_all[j, :, k].reshape(rows, HD)
            scores = lax.dot_general(
                q_rows,
                cache_buf[:, pl.ds(key_at, HD)],
                (((1,), (1,)), ((), ())),
                preferred_element_type=jnp.float32,
            )
            scores = scores * TOKEN_LOG2 + bias_buf[...]
            peak = jnp.max(scores, axis=1, keepdims=True)
            weights = jnp.exp2(scores - jnp.maximum(peak, 0.1 * NEGATIVE))
            total = jnp.sum(weights, axis=1, keepdims=True)
            partial = jnp.dot(
                weights.astype(jnp.bfloat16),
                cache_buf[:, pl.ds(value_at, HD)],
                preferred_element_type=jnp.float32,
            ).astype(jnp.bfloat16)
            tile = jnp.where(lane == 0, peak, total).T[:8]
            if j == 0:
                part_tp[0, k] = partial
                stat_tp[0, k] = tile
            else:
                part_send[j, k] = partial
                stat_send[j, k] = tile
        if j > 0:
            target = {"tp": tp_from(j)}
            stats[j] = remote(
                stat_send.at[j], stat_tp.at[j], st_send.at[j], st_recv.at[j], target
            )
            parts[j] = remote(
                part_send.at[j], part_tp.at[j], pt_send.at[j], pt_recv.at[j], target
            )

    for j in range(1, nt):
        stats[j].wait_recv()
        parts[j].wait_recv()

    def columns_of(pieces):
        height = -(-len(pieces) // 8) * 8
        index = lax.broadcasted_iota(jnp.int32, (height, rows), 0)
        tile = jnp.zeros((height, rows), jnp.float32)
        for i, piece in enumerate(pieces):
            tile = jnp.where(index == i, piece, tile)
        return tile.T

    for k in range(kv_local):
        peaks = [stat_tp[j, k, 0:1, :] for j in range(nt)]
        top = peaks[0]
        for piece in peaks[1:]:
            top = jnp.maximum(top, piece)
        scale = [jnp.exp2(piece - top) for piece in peaks]
        total = scale[0] * stat_tp[0, k, 1:2, :]
        for j in range(1, nt):
            total += scale[j] * stat_tp[j, k, 1:2, :]
        spread_scale = columns_of(scale)
        joined = spread_scale[:, 0:1] * part_tp[0, k].astype(jnp.float32)
        for j in range(1, nt):
            joined += spread_scale[:, j : j + 1] * part_tp[j, k].astype(jnp.float32)
        joined = joined.astype(jnp.bfloat16)
        index = lax.broadcasted_iota(jnp.int32, (8, rows), 0)
        tile = jnp.where(index == 0, top, total)
        z_stat_send[k] = tile
        z_stat[0, k] = tile
        z_part[0, k] = joined[:sub]
        for a in range(1, nz):
            z_send[a, k] = joined[a * sub : (a + 1) * sub]
    from_z = {}
    for a in reversed(z_order):
        target = {"kvb": z_back(a)}
        from_z[a] = (
            remote(z_stat_send, z_stat.at[a], zs_send.at[a], zs_recv.at[a], target),
            remote(z_send.at[a], z_part.at[a], zp_send.at[a], zp_recv.at[a], target),
        )
    for a in z_order:
        for copy in from_z[a]:
            copy.wait_recv()

    for k in range(kv_local):
        spread_stat = columns_of([z_stat[a, k, i : i + 1, :] for a in range(nz) for i in range(2)])
        peaks = [spread_stat[a * sub : (a + 1) * sub, 2 * a : 2 * a + 1] for a in range(nz)]
        sums = [spread_stat[a * sub : (a + 1) * sub, 2 * a + 1 : 2 * a + 2] for a in range(nz)]
        top = fresh[k]
        for piece in peaks:
            top = jnp.maximum(top, piece)
        denominator = jnp.exp2(fresh[k] - top)
        numerator = denominator * new_buf[k, 1]
        for a in range(nz):
            scale = jnp.exp2(peaks[a] - top)
            denominator += scale * sums[a]
            numerator += scale * z_part[a, k].astype(jnp.float32)
        row_buf[k] = numerator / denominator
        for q in range(per_kv):
            head = k * per_kv + q
            lhs_buf[0:seq_rep, head * HD : (head + 1) * HD] = row_buf[
                k, q * seq_rep : (q + 1) * seq_rep, :
            ]
    attended = lhs_buf[...].astype(jnp.bfloat16)

    step = min(512, width)
    reduced = {}
    for j in far_first + [0]:
        weight_copies[j].wait()

        def column_step(i, carry, j=j):
            at = pl.ds(pl.multiple_of(i * step, LANES), step)
            got = jnp.dot(attended, weight_buf[j, :, at], preferred_element_type=jnp.float32)
            proj_send[j, :, at] = got[:seq_rep]
            return carry

        lax.fori_loop(0, width // step, column_step, 0)
        if j > 0:
            reduced[j] = remote(
                proj_send.at[j],
                proj_recv.at[j],
                rs_send.at[j],
                rs_recv.at[j],
                {"tp": tp_to(j)},
            )
    own = pl.ds(pl.multiple_of(t * width, LANES), width)
    summed = proj_send[0]
    for j in far_first:
        reduced[j].wait_recv()
        summed += proj_recv[j]
    stream = (residual_ref[:, own].astype(jnp.float32) + summed).astype(jnp.bfloat16)
    stream_ref[...] = stream
    stream_wide = stream.astype(jnp.float32)
    square = jnp.sum(stream_wide * stream_wide, axis=1, keepdims=True)
    ss_send[...] = jnp.broadcast_to(square, ss_send.shape)
    squares = [
        remote(ss_send, ss_recv.at[j], sq_send.at[j], sq_recv.at[j], {"tp": tp_to(j)})
        for j in far_first
    ]
    gain = gain_ref[...].astype(jnp.float32)
    for copy in squares:
        copy.wait_recv()
    for j in range(1, nt):
        square += ss_recv[j][:, 0:1]
    mean_square = square * (1.0 / (width * nt))
    normed_ref[...] = (stream_wide * lax.rsqrt(mean_square + EPSILON) * gain).astype(jnp.bfloat16)
    for copy in pending:
        copy.wait_send()


def on_device(
    residual,
    queries,
    new_kv,
    kv_cache,
    lengths,
    slot_seq,
    slot_block,
    block_counts,
    out_weight,
    norm_gain,
):
    nt = lax.axis_size("tp")
    nz = lax.axis_size("kvb")
    seq_rep = residual.shape[0]
    local_heads = queries.shape[1] // HD
    kv_local = max(1, local_heads // GROUP_HEADS)
    sub = local_heads // kv_local * seq_rep
    rows = nz * sub
    slots = kv_cache.shape[0]
    tokens = slots * BLK
    width = norm_gain.shape[0]
    depth = out_weight.shape[0]
    bf16, f32 = jnp.bfloat16, jnp.float32
    dma = pltpu.SemaphoreType.DMA
    vmem = pl.BlockSpec(memory_space=pltpu.VMEM)
    smem = pl.BlockSpec(memory_space=pltpu.SMEM)
    hbm = pl.BlockSpec(memory_space=pl.ANY)

    def body(*refs):
        kernel(nz, nt, seq_rep, local_heads, *refs)

    return pl.pallas_call(
        body,
        out_shape=(
            jax.ShapeDtypeStruct((seq_rep, width), bf16),
            jax.ShapeDtypeStruct((seq_rep, width), bf16),
        ),
        in_specs=[smem, smem, vmem, vmem, vmem, vmem, vmem, vmem, hbm, hbm],
        out_specs=(vmem, vmem),
        scratch_shapes=[
            pltpu.VMEM((tokens, kv_cache.shape[2]), bf16),
            pltpu.VMEM((nt, depth, width), bf16),
            pltpu.VMEM((rows, tokens), f32),
            pltpu.VMEM((kv_local, sub, HD), f32),
            pltpu.VMEM((kv_local, 2, sub, HD), f32),
            pltpu.VMEM((nt, nz, kv_local, sub, HD), bf16),
            pltpu.VMEM((nt, kv_local, rows, HD), bf16),
            pltpu.VMEM((nt, kv_local, 8, rows), f32),
            pltpu.VMEM((nt, kv_local, rows, HD), bf16),
            pltpu.VMEM((nt, kv_local, 8, rows), f32),
            pltpu.VMEM((nz, kv_local, sub, HD), bf16),
            pltpu.VMEM((kv_local, 8, rows), f32),
            pltpu.VMEM((nz, kv_local, sub, HD), bf16),
            pltpu.VMEM((nz, kv_local, 8, rows), f32),
            pltpu.VMEM((16, depth), f32),
            pltpu.VMEM((nt, seq_rep, width), f32),
            pltpu.VMEM((nt, seq_rep, width), f32),
            pltpu.VMEM((seq_rep, LANES), f32),
            pltpu.VMEM((nt, seq_rep, LANES), f32),
            dma,
            dma((nt,)),
            dma((nz,)),
            dma((nz,)),
            dma((nz, nt)),
            dma((nz, nt)),
            dma((nt,)),
            dma((nt,)),
            dma((nt,)),
            dma((nt,)),
            dma((nz,)),
            dma((nz,)),
            dma((nz,)),
            dma((nz,)),
            dma((nt,)),
            dma((nt,)),
            dma((nt,)),
            dma((nt,)),
        ],
        compiler_params=pltpu.CompilerParams(
            collective_id=0, has_side_effects=True, vmem_limit_bytes=62 * 1024 * 1024
        ),
    )(
        lengths,
        block_counts,
        slot_seq.reshape(1, slots),
        slot_block.reshape(1, slots),
        residual,
        queries,
        new_kv,
        norm_gain.reshape(1, width),
        kv_cache.reshape(tokens, kv_cache.shape[2]),
        out_weight,
    )


def solution(mesh):
    placed = (
        P(("groups", "kvb"), None),
        P(("groups", "kvb"), "tp"),
        P(("groups", "kvb"), None),
        P(("groups", "kvb", "tp"), None, None),
        P("groups"),
        P(("groups", "kvb", "tp")),
        P(("groups", "kvb", "tp")),
        P(("groups", "kvb", "tp")),
        P("tp", None),
        P("tp"),
    )
    return jax.shard_map(
        on_device,
        mesh=mesh,
        in_specs=placed,
        out_specs=(P(("groups", "kvb"), "tp"), P(("groups", "kvb"), "tp")),
        check_vma=False,
    )
```

```python
import math

import jax
import jax.numpy as jnp
from jax import lax
from jax.experimental import pallas as pl
from jax.experimental.pallas import tpu as pltpu
from jax.sharding import PartitionSpec as P

QH = 64
KVH = 8
HD = 128
BLK = 16
GROUP_HEADS = QH // KVH

NEGATIVE = -1e30
EPSILON = 1e-06
LANES = 128
TOKEN_LOG2 = math.log2(math.e) * HD ** (-0.5)
MESH = pl.DeviceIdType.MESH


def kernel(
    nz,
    nt,
    seq_rep,
    local_heads,
    lengths_ref,
    counts_ref,
    slot_seq_hbm,
    slot_block_hbm,
    residual_hbm,
    queries_hbm,
    new_kv_hbm,
    gain_hbm,
    cache_ref,
    weight_ref,
    stream_ref,
    factor_ref,
    slot_seq_ref,
    slot_block_ref,
    residual_ref,
    queries_ref,
    new_kv_ref,
    gain_ref,
    cache_buf,
    weight_buf,
    bias_buf,
    row_buf,
    new_buf,
    q_all,
    part_tp,
    stat_tp,
    part_send,
    stat_send,
    z_send,
    z_stat_send,
    z_part,
    z_stat,
    lhs_buf,
    proj_send,
    proj_recv,
    ss_send,
    ss_recv,
    input_sem,
    cache_sem,
    weight_sem,
    qz_send,
    qz_recv,
    qt_send,
    qt_recv,
    pt_send,
    pt_recv,
    st_send,
    st_recv,
    zp_send,
    zp_recv,
    zs_send,
    zs_recv,
    rs_send,
    rs_recv,
    sq_send,
    sq_recv,
):
    z = lax.axis_index("kvb")
    t = lax.axis_index("tp")
    kv_local = max(1, local_heads // GROUP_HEADS)
    per_kv = local_heads // kv_local
    sub = per_kv * seq_rep
    rows = nz * sub
    tokens = cache_buf.shape[0]
    slots = slot_seq_ref.shape[1]
    width = stream_ref.shape[1]
    fast = 2 if nt % 2 == 0 else 1
    slow = nt // fast

    def tp_to(j):
        return lax.rem(t // fast + j // fast, slow) * fast + lax.rem(t % fast + j % fast, fast)

    def tp_from(j):
        back = (slow - j // fast) % slow
        back_fast = (fast - j % fast) % fast
        return lax.rem(t // fast + back, slow) * fast + lax.rem(t % fast + back_fast, fast)

    def z_to(a):
        return lax.rem(z + a, nz)

    def z_back(a):
        return lax.rem(z + (nz - a), nz)

    far_first = sorted(range(1, nt), key=lambda j: (j < fast, j))

    barrier = pltpu.get_barrier_semaphore()
    for a in range(1, nz):
        pl.semaphore_signal(barrier, inc=1, device_id={"kvb": z_to(a)}, device_id_type=MESH)
    for j in range(1, nt):
        pl.semaphore_signal(barrier, inc=1, device_id={"tp": tp_to(j)}, device_id_type=MESH)

    own = pl.ds(pl.multiple_of(t * width, LANES), width)
    inputs = [
        pltpu.make_async_copy(src, dst, input_sem.at[i])
        for i, (src, dst) in enumerate(
            (
                (queries_hbm, queries_ref),
                (slot_seq_hbm, slot_seq_ref),
                (slot_block_hbm, slot_block_ref),
                (new_kv_hbm, new_kv_ref),
                (residual_hbm.at[:, own], residual_ref),
                (gain_hbm, gain_ref),
            )
        )
    ]
    for copy in inputs:
        copy.start()
    cache_copy = pltpu.make_async_copy(cache_ref, cache_buf, cache_sem)
    cache_copy.start()
    inputs[0].wait()

    wide_q = queries_ref[...].astype(jnp.float32)
    for k in range(kv_local):
        for q in range(per_kv):
            head = k * per_kv + q
            row_buf[k, q * seq_rep : (q + 1) * seq_rep, :] = wide_q[:, head * HD : (head + 1) * HD]
    for k in range(kv_local):
        q_all[0, 0, k] = row_buf[k].astype(jnp.bfloat16)
    with jax.named_scope("barrier_wait"):
        pl.semaphore_wait(barrier, nz - 1 + nt - 1)

    pending = []

    def remote(src, dst, send, recv, target):
        copy = pltpu.make_async_remote_copy(
            src_ref=src,
            dst_ref=dst,
            send_sem=send,
            recv_sem=recv,
            device_id=target,
            device_id_type=MESH,
        )
        copy.start()
        pending.append(copy)
        return copy

    z_order = sorted(range(1, nz), key=lambda a: min(a, nz - a))
    q_from_z = {}
    for a in reversed(z_order):
        q_from_z[a] = remote(
            q_all.at[0, 0], q_all.at[0, a], qz_send.at[a], qz_recv.at[a], {"kvb": z_to(a)}
        )
    q_from_tp = {}

    def forward(a):
        for j in far_first:
            q_from_tp[a, j] = remote(
                q_all.at[0, a],
                q_all.at[j, a],
                qt_send.at[a, j],
                qt_recv.at[a, j],
                {"tp": tp_to(j)},
            )

    forward(0)

    depth = weight_buf.shape[0] // kv_local
    pieces = 4
    weight_copies = []
    for i in range(kv_local * pieces):
        part_rows = pl.ds(i * (depth // pieces), depth // pieces)
        weight_copies.append(
            pltpu.make_async_copy(
                weight_ref.at[part_rows, :], weight_buf.at[part_rows, :], weight_sem.at[i]
            )
        )
        weight_copies[i].start()
    for copy in inputs[1:]:
        copy.wait()

    row_id = lax.broadcasted_iota(jnp.int32, (rows, slots), 0)
    slot_id = lax.broadcasted_iota(jnp.int32, (rows, slots), 1)
    row_seq = lax.rem(z + nz - row_id // sub, nz) * seq_rep + lax.rem(row_id, seq_rep)
    row_len = jnp.zeros((rows, slots), jnp.int32)
    for s in range(nz * seq_rep):
        row_len = jnp.where(row_seq == s, lengths_ref[s], row_len)
    held = (row_seq == slot_seq_ref[...]) & (slot_id < counts_ref[0])
    limit = jnp.where(held, jnp.clip(row_len - BLK * slot_block_ref[...], 0, BLK), 0)
    token_slot = lax.broadcasted_iota(jnp.int32, (slots, tokens), 1) // BLK
    spread = (token_slot == lax.broadcasted_iota(jnp.int32, (slots, tokens), 0)).astype(jnp.float32)
    reach = jnp.dot(
        limit.astype(jnp.float32).astype(jnp.bfloat16),
        spread.astype(jnp.bfloat16),
        preferred_element_type=jnp.float32,
    )
    offset = lax.rem(lax.broadcasted_iota(jnp.int32, (rows, tokens), 1), BLK).astype(jnp.float32)
    bias_buf[...] = jnp.where(offset < reach, 0.0, NEGATIVE)

    own_kv = t * local_heads // GROUP_HEADS
    fresh = []
    for k in range(kv_local):
        for part in range(2):
            at = pl.multiple_of((part * KVH + own_kv + k) * HD, LANES)
            piece = new_kv_ref[:, pl.ds(at, HD)].astype(jnp.float32)
            for q in range(per_kv):
                new_buf[k, part, q * seq_rep : (q + 1) * seq_rep, :] = piece
        fresh.append(jnp.sum(row_buf[k] * new_buf[k, 0], axis=1, keepdims=True) * TOKEN_LOG2)
    lhs_buf[...] = jnp.zeros_like(lhs_buf)

    for a in z_order:
        with jax.named_scope(f"q_z_wait{a}"):
            q_from_z[a].wait_recv()
        forward(a)

    with jax.named_scope("cache_wait"):
        cache_copy.wait()
    lane = lax.broadcasted_iota(jnp.int32, (rows, LANES), 1)
    copies = {}

    def attend(j, k):
        first_kv = tp_from(j) * local_heads // GROUP_HEADS
        key_at = pl.multiple_of((first_kv + k) * HD, LANES)
        value_at = pl.multiple_of((KVH + first_kv + k) * HD, LANES)
        q_rows = q_all[j, :, k].reshape(rows, HD)
        scores = lax.dot_general(
            q_rows,
            cache_buf[:, pl.ds(key_at, HD)],
            (((1,), (1,)), ((), ())),
            preferred_element_type=jnp.float32,
        )
        scores = scores * TOKEN_LOG2 + bias_buf[...]
        peak = jnp.max(scores, axis=1, keepdims=True)
        weights = jnp.exp2(scores - jnp.maximum(peak, 0.1 * NEGATIVE))
        total = jnp.sum(weights, axis=1, keepdims=True)
        partial = jnp.dot(
            weights.astype(jnp.bfloat16),
            cache_buf[:, pl.ds(value_at, HD)],
            preferred_element_type=jnp.float32,
        ).astype(jnp.bfloat16)
        tile = jnp.where(lane == 0, peak, total).T[:8]
        if j == 0:
            part_tp[0, k] = partial
            stat_tp[0, k] = tile
            return
        part_send[j, k] = partial
        stat_send[j, k] = tile
        target = {"tp": tp_from(j)}
        copies[j, k] = (
            remote(
                stat_send.at[j, k],
                stat_tp.at[j, k],
                st_send.at[j, k],
                st_recv.at[j, k],
                target,
            ),
            remote(
                part_send.at[j, k],
                part_tp.at[j, k],
                pt_send.at[j, k],
                pt_recv.at[j, k],
                target,
            ),
        )

    for k in range(kv_local):
        attend(0, k)
    arrived = set()
    for k in range(kv_local):
        for j in far_first if k == kv_local - 1 else range(1, nt):
            if j not in arrived:
                arrived.add(j)
                with jax.named_scope(f"q_tp_wait{j}"):
                    for a in range(nz):
                        q_from_tp[a, j].wait_recv()
            attend(j, k)

    def columns_of(pieces):
        height = -(-len(pieces) // 8) * 8
        index = lax.broadcasted_iota(jnp.int32, (height, rows), 0)
        tile = jnp.zeros((height, rows), jnp.float32)
        for i, piece in enumerate(pieces):
            tile = jnp.where(index == i, piece, tile)
        return tile.T

    from_z = {}
    for k in range(kv_local):
        with jax.named_scope(f"part_wait{k}"):
            for j in range(1, nt):
                for copy in copies[j, k]:
                    copy.wait_recv()
        peaks = [stat_tp[j, k, 0:1, :] for j in range(nt)]
        top = peaks[0]
        for piece in peaks[1:]:
            top = jnp.maximum(top, piece)
        scale = [jnp.exp2(piece - top) for piece in peaks]
        total = scale[0] * stat_tp[0, k, 1:2, :]
        for j in range(1, nt):
            total += scale[j] * stat_tp[j, k, 1:2, :]
        spread_scale = columns_of(scale)
        joined = spread_scale[:, 0:1] * part_tp[0, k].astype(jnp.float32)
        for j in range(1, nt):
            joined += spread_scale[:, j : j + 1] * part_tp[j, k].astype(jnp.float32)
        joined = joined.astype(jnp.bfloat16)
        index = lax.broadcasted_iota(jnp.int32, (8, rows), 0)
        tile = jnp.where(index == 0, top, total)
        z_stat_send[k] = tile
        z_stat[0, k] = tile
        z_part[0, k] = joined[:sub]
        for a in range(1, nz):
            z_send[a, k] = joined[a * sub : (a + 1) * sub]
        for a in reversed(z_order):
            target = {"kvb": z_back(a)}
            from_z[a, k] = (
                remote(
                    z_stat_send.at[k],
                    z_stat.at[a, k],
                    zs_send.at[a, k],
                    zs_recv.at[a, k],
                    target,
                ),
                remote(
                    z_send.at[a, k],
                    z_part.at[a, k],
                    zp_send.at[a, k],
                    zp_recv.at[a, k],
                    target,
                ),
            )

    step = min(1024, width)
    reduced = {}
    for k in range(kv_local):
        with jax.named_scope(f"z_wait{k}"):
            for a in z_order:
                for copy in from_z[a, k]:
                    copy.wait_recv()
        spread_stat = columns_of([z_stat[a, k, i : i + 1, :] for a in range(nz) for i in range(2)])
        peaks = [spread_stat[a * sub : (a + 1) * sub, 2 * a : 2 * a + 1] for a in range(nz)]
        sums = [spread_stat[a * sub : (a + 1) * sub, 2 * a + 1 : 2 * a + 2] for a in range(nz)]
        top = fresh[k]
        for piece in peaks:
            top = jnp.maximum(top, piece)
        denominator = jnp.exp2(fresh[k] - top)
        numerator = denominator * new_buf[k, 1]
        for a in range(nz):
            scale = jnp.exp2(peaks[a] - top)
            denominator += scale * sums[a]
            numerator += scale * z_part[a, k].astype(jnp.float32)
        row_buf[k] = numerator / denominator
        for q in range(per_kv):
            lhs_buf[k, 0:seq_rep, q * HD : (q + 1) * HD] = row_buf[
                k, q * seq_rep : (q + 1) * seq_rep, :
            ]
        attended = lhs_buf[k].astype(jnp.bfloat16)
        with jax.named_scope(f"weight_wait{k}"):
            for copy in weight_copies[k * pieces : (k + 1) * pieces]:
                copy.wait()
        for j in far_first + [0]:
            column = tp_to(j) * width

            def column_step(i, carry, j=j, k=k, column=column, attended=attended):
                at = pl.ds(pl.multiple_of(i * step, LANES), step)
                source = pl.ds(pl.multiple_of(column + i * step, LANES), step)
                got = jnp.dot(
                    attended,
                    weight_buf[k * depth : (k + 1) * depth, source],
                    preferred_element_type=jnp.float32,
                )[:seq_rep]
                if k > 0:
                    got += proj_send[j, :, at]
                proj_send[j, :, at] = got
                return carry

            lax.fori_loop(0, width // step, column_step, 0)
            if j > 0 and k == kv_local - 1:
                reduced[j] = remote(
                    proj_send.at[j],
                    proj_recv.at[j],
                    rs_send.at[j],
                    rs_recv.at[j],
                    {"tp": tp_to(j)},
                )
    summed = proj_send[0]
    with jax.named_scope("sum_wait"):
        for j in far_first:
            reduced[j].wait_recv()
    for j in far_first:
        summed += proj_recv[j]
    stream = (residual_ref[...].astype(jnp.float32) + summed).astype(jnp.bfloat16)
    stream_wide = stream.astype(jnp.float32)
    stream_ref[...] = stream_wide
    square = jnp.sum(stream_wide * stream_wide, axis=1, keepdims=True)
    ss_send[...] = jnp.broadcast_to(square, ss_send.shape)
    squares = [
        remote(ss_send, ss_recv.at[j], sq_send.at[j], sq_recv.at[j], {"tp": tp_to(j)})
        for j in far_first
    ]
    gain = gain_ref[...].astype(jnp.float32).reshape(1, width)
    with jax.named_scope("square_wait"):
        for copy in squares:
            copy.wait_recv()
    for j in range(1, nt):
        square += ss_recv[j][:, 0:1]
    mean_square = square * (1.0 / (width * nt))
    factor_ref[...] = lax.rsqrt(mean_square + EPSILON) * gain
    for copy in pending:
        copy.wait_send()


def on_device(
    residual,
    queries,
    new_kv,
    kv_cache,
    lengths,
    slot_seq,
    slot_block,
    block_counts,
    out_weight,
    norm_gain,
):
    nt = lax.axis_size("tp")
    nz = lax.axis_size("kvb")
    seq_rep = residual.shape[0]
    local_heads = queries.shape[1] // HD
    kv_local = max(1, local_heads // GROUP_HEADS)
    sub = local_heads // kv_local * seq_rep
    rows = nz * sub
    slots = kv_cache.shape[0]
    tokens = slots * BLK
    width = norm_gain.shape[0]
    depth = out_weight.shape[0]
    bf16, f32 = jnp.bfloat16, jnp.float32
    dma = pltpu.SemaphoreType.DMA
    vmem = pl.BlockSpec(memory_space=pltpu.VMEM)
    smem = pl.BlockSpec(memory_space=pltpu.SMEM)
    hbm = pl.BlockSpec(memory_space=pl.ANY)

    def body(*refs):
        kernel(nz, nt, seq_rep, local_heads, *refs)

    stream, factor = pl.pallas_call(
        body,
        out_shape=(
            jax.ShapeDtypeStruct((seq_rep, width), f32),
            jax.ShapeDtypeStruct((seq_rep, width), f32),
        ),
        in_specs=[smem, smem] + [hbm] * 8,
        out_specs=(vmem, vmem),
        scratch_shapes=[
            pltpu.VMEM((1, slots), jnp.int32),
            pltpu.VMEM((1, slots), jnp.int32),
            pltpu.VMEM((seq_rep, width), bf16),
            pltpu.VMEM(queries.shape, bf16),
            pltpu.VMEM(new_kv.shape, bf16),
            pltpu.VMEM((width,), bf16),
            pltpu.VMEM((tokens, kv_cache.shape[2]), bf16),
            pltpu.VMEM(out_weight.shape, bf16),
            pltpu.VMEM((rows, tokens), f32),
            pltpu.VMEM((kv_local, sub, HD), f32),
            pltpu.VMEM((kv_local, 2, sub, HD), f32),
            pltpu.VMEM((nt, nz, kv_local, sub, HD), bf16),
            pltpu.VMEM((nt, kv_local, rows, HD), bf16),
            pltpu.VMEM((nt, kv_local, 8, rows), f32),
            pltpu.VMEM((nt, kv_local, rows, HD), bf16),
            pltpu.VMEM((nt, kv_local, 8, rows), f32),
            pltpu.VMEM((nz, kv_local, sub, HD), bf16),
            pltpu.VMEM((kv_local, 8, rows), f32),
            pltpu.VMEM((nz, kv_local, sub, HD), bf16),
            pltpu.VMEM((nz, kv_local, 8, rows), f32),
            pltpu.VMEM((kv_local, 16, depth // kv_local), f32),
            pltpu.VMEM((nt, seq_rep, width), f32),
            pltpu.VMEM((nt, seq_rep, width), f32),
            pltpu.VMEM((seq_rep, LANES), f32),
            pltpu.VMEM((nt, seq_rep, LANES), f32),
            dma((6,)),
            dma,
            dma((kv_local * 4,)),
            dma((nz,)),
            dma((nz,)),
            dma((nz, nt)),
            dma((nz, nt)),
            dma((nt, kv_local)),
            dma((nt, kv_local)),
            dma((nt, kv_local)),
            dma((nt, kv_local)),
            dma((nz, kv_local)),
            dma((nz, kv_local)),
            dma((nz, kv_local)),
            dma((nz, kv_local)),
            dma((nt,)),
            dma((nt,)),
            dma((nt,)),
            dma((nt,)),
        ],
        compiler_params=pltpu.CompilerParams(
            collective_id=0, has_side_effects=True, vmem_limit_bytes=62 * 1024 * 1024
        ),
    )(
        lengths,
        block_counts,
        slot_seq.reshape(1, slots),
        slot_block.reshape(1, slots),
        residual,
        queries,
        new_kv,
        norm_gain,
        kv_cache.reshape(tokens, kv_cache.shape[2]),
        out_weight,
    )
    return (stream.astype(bf16), (stream * factor).astype(bf16))


def solution(mesh):
    placed = (
        P(("groups", "kvb"), None),
        P(("groups", "kvb"), "tp"),
        P(("groups", "kvb"), None),
        P(("groups", "kvb", "tp"), None, None),
        P("groups"),
        P(("groups", "kvb", "tp")),
        P(("groups", "kvb", "tp")),
        P(("groups", "kvb", "tp")),
        P("tp", None),
        P("tp"),
    )
    return jax.shard_map(
        on_device,
        mesh=mesh,
        in_specs=placed,
        out_specs=(P(("groups", "kvb"), "tp"), P(("groups", "kvb"), "tp")),
        check_vma=False,
    )
```

```python
import math

import jax
import jax.numpy as jnp
from jax import lax
from jax.experimental import pallas as pl
from jax.experimental.pallas import tpu as pltpu
from jax.sharding import PartitionSpec as P

QH = 64
KVH = 8
HD = 128
BLK = 16
GROUP_HEADS = QH // KVH

NEGATIVE = -1e30
EPSILON = 1e-06
LANES = 128
TOKEN_LOG2 = math.log2(math.e) * HD ** (-0.5)
MESH = pl.DeviceIdType.MESH


def kernel(
    nz,
    nt,
    seq_rep,
    local_heads,
    lengths_ref,
    counts_ref,
    slot_seq_hbm,
    slot_block_hbm,
    residual_hbm,
    queries_hbm,
    new_kv_hbm,
    gain_hbm,
    cache_ref,
    weight_ref,
    stream_ref,
    factor_ref,
    slot_seq_ref,
    slot_block_ref,
    residual_ref,
    queries_ref,
    new_kv_ref,
    gain_ref,
    cache_buf,
    weight_buf,
    bias_buf,
    row_buf,
    new_buf,
    q_all,
    part_tp,
    stat_tp,
    part_send,
    stat_send,
    z_send,
    z_stat_send,
    z_part,
    z_stat,
    lhs_buf,
    proj_sum,
    proj_send,
    proj_recv,
    ss_send,
    ss_recv,
    input_sem,
    cache_sem,
    weight_sem,
    qz_send,
    qz_recv,
    qt_send,
    qt_recv,
    pt_send,
    pt_recv,
    st_send,
    st_recv,
    zp_send,
    zp_recv,
    zs_send,
    zs_recv,
    rs_send,
    rs_recv,
    sq_send,
    sq_recv,
):
    z = lax.axis_index("kvb")
    t = lax.axis_index("tp")
    kv_local = max(1, local_heads // GROUP_HEADS)
    per_kv = local_heads // kv_local
    sub = per_kv * seq_rep
    rows = nz * sub
    tokens = cache_buf.shape[0]
    slots = slot_seq_ref.shape[1]
    width = stream_ref.shape[1]
    fast = 2 if nt % 2 == 0 else 1
    slow = nt // fast

    def tp_to(j):
        return lax.rem(t // fast + j // fast, slow) * fast + lax.rem(t % fast + j % fast, fast)

    def tp_from(j):
        back = (slow - j // fast) % slow
        back_fast = (fast - j % fast) % fast
        return lax.rem(t // fast + back, slow) * fast + lax.rem(t % fast + back_fast, fast)

    def z_to(a):
        return lax.rem(z + a, nz)

    def z_back(a):
        return lax.rem(z + (nz - a), nz)

    far_first = sorted(range(1, nt), key=lambda j: (j < fast, j))

    barrier = pltpu.get_barrier_semaphore()
    for a in range(1, nz):
        pl.semaphore_signal(barrier, inc=1, device_id={"kvb": z_to(a)}, device_id_type=MESH)
    for j in range(1, nt):
        pl.semaphore_signal(barrier, inc=1, device_id={"tp": tp_to(j)}, device_id_type=MESH)

    own = pl.ds(pl.multiple_of(t * width, LANES), width)
    inputs = [
        pltpu.make_async_copy(src, dst, input_sem.at[i])
        for i, (src, dst) in enumerate(
            (
                (queries_hbm, queries_ref),
                (slot_seq_hbm, slot_seq_ref),
                (slot_block_hbm, slot_block_ref),
                (new_kv_hbm, new_kv_ref),
                (residual_hbm.at[:, own], residual_ref),
                (gain_hbm, gain_ref),
            )
        )
    ]
    for copy in inputs:
        copy.start()
    cache_copy = pltpu.make_async_copy(cache_ref, cache_buf, cache_sem)
    cache_copy.start()
    inputs[0].wait()

    wide_q = queries_ref[...].astype(jnp.float32)
    for k in range(kv_local):
        for q in range(per_kv):
            head = k * per_kv + q
            row_buf[k, q * seq_rep : (q + 1) * seq_rep, :] = wide_q[:, head * HD : (head + 1) * HD]
    for k in range(kv_local):
        q_all[0, 0, k] = row_buf[k].astype(jnp.bfloat16)
    with jax.named_scope("barrier_wait"):
        pl.semaphore_wait(barrier, nz - 1 + nt - 1)

    pending = []

    def remote(src, dst, send, recv, target):
        copy = pltpu.make_async_remote_copy(
            src_ref=src,
            dst_ref=dst,
            send_sem=send,
            recv_sem=recv,
            device_id=target,
            device_id_type=MESH,
        )
        copy.start()
        pending.append(copy)
        return copy

    z_order = sorted(range(1, nz), key=lambda a: min(a, nz - a))
    q_from_z = {}
    for a in reversed(z_order):
        q_from_z[a] = remote(
            q_all.at[0, 0], q_all.at[0, a], qz_send.at[a], qz_recv.at[a], {"kvb": z_to(a)}
        )
    q_from_tp = {}

    def relayed(j):
        return fast == 2 and j > 2 and j % 2 == 1

    def relay(j):
        for a in [0] + z_order:
            with jax.named_scope(f"q_relay_wait{j}"):
                q_from_tp[a, j].wait_recv()
            q_from_tp[a, j + 1] = remote(
                q_all.at[j, a],
                q_all.at[j + 1, a],
                qt_send.at[a, j + 1],
                qt_recv.at[a, j + 1],
                {"tp": tp_to(1)},
            )

    def forward(a):
        for j in far_first:
            if relayed(j):
                continue
            q_from_tp[a, j] = remote(
                q_all.at[0, a],
                q_all.at[j, a],
                qt_send.at[a, j],
                qt_recv.at[a, j],
                {"tp": tp_to(j)},
            )

    forward(0)

    depth = weight_buf.shape[0] // kv_local
    pieces = 4
    weight_copies = []
    for i in range(kv_local * pieces):
        part_rows = pl.ds(i * (depth // pieces), depth // pieces)
        weight_copies.append(
            pltpu.make_async_copy(
                weight_ref.at[part_rows, :], weight_buf.at[part_rows, :], weight_sem.at[i]
            )
        )
        weight_copies[i].start()
    for copy in inputs[1:]:
        copy.wait()

    row_id = lax.broadcasted_iota(jnp.int32, (rows, slots), 0)
    slot_id = lax.broadcasted_iota(jnp.int32, (rows, slots), 1)
    row_seq = lax.rem(z + nz - row_id // sub, nz) * seq_rep + lax.rem(row_id, seq_rep)
    row_len = jnp.zeros((rows, slots), jnp.int32)
    for s in range(nz * seq_rep):
        row_len = jnp.where(row_seq == s, lengths_ref[s], row_len)
    held = (row_seq == slot_seq_ref[...]) & (slot_id < counts_ref[0])
    limit = jnp.where(held, jnp.clip(row_len - BLK * slot_block_ref[...], 0, BLK), 0)
    token_slot = lax.broadcasted_iota(jnp.int32, (slots, tokens), 1) // BLK
    spread = (token_slot == lax.broadcasted_iota(jnp.int32, (slots, tokens), 0)).astype(jnp.float32)
    reach = jnp.dot(
        limit.astype(jnp.float32).astype(jnp.bfloat16),
        spread.astype(jnp.bfloat16),
        preferred_element_type=jnp.float32,
    )
    offset = lax.rem(lax.broadcasted_iota(jnp.int32, (rows, tokens), 1), BLK).astype(jnp.float32)
    bias_buf[...] = jnp.where(offset < reach, 0.0, NEGATIVE)

    own_kv = t * local_heads // GROUP_HEADS
    fresh = []
    for k in range(kv_local):
        for part in range(2):
            at = pl.multiple_of((part * KVH + own_kv + k) * HD, LANES)
            piece = new_kv_ref[:, pl.ds(at, HD)].astype(jnp.float32)
            for q in range(per_kv):
                new_buf[k, part, q * seq_rep : (q + 1) * seq_rep, :] = piece
        fresh.append(jnp.sum(row_buf[k] * new_buf[k, 0], axis=1, keepdims=True) * TOKEN_LOG2)
    lhs_buf[...] = jnp.zeros_like(lhs_buf)

    for a in z_order:
        with jax.named_scope(f"q_z_wait{a}"):
            q_from_z[a].wait_recv()
        forward(a)

    with jax.named_scope("cache_wait"):
        cache_copy.wait()
    lane = lax.broadcasted_iota(jnp.int32, (rows, LANES), 1)
    copies = {}

    def attend(j, k):
        first_kv = tp_from(j) * local_heads // GROUP_HEADS
        key_at = pl.multiple_of((first_kv + k) * HD, LANES)
        value_at = pl.multiple_of((KVH + first_kv + k) * HD, LANES)
        q_rows = q_all[j, :, k].reshape(rows, HD)
        scores = lax.dot_general(
            q_rows,
            cache_buf[:, pl.ds(key_at, HD)],
            (((1,), (1,)), ((), ())),
            preferred_element_type=jnp.float32,
        )
        scores = scores * TOKEN_LOG2 + bias_buf[...]
        peak = jnp.max(scores, axis=1, keepdims=True)
        weights = jnp.exp2(scores - jnp.maximum(peak, 0.1 * NEGATIVE))
        total = jnp.sum(weights, axis=1, keepdims=True)
        partial = jnp.dot(
            weights.astype(jnp.bfloat16),
            cache_buf[:, pl.ds(value_at, HD)],
            preferred_element_type=jnp.float32,
        ).astype(jnp.bfloat16)
        tile = jnp.where(lane == 0, peak, total).T[:8]
        if j == 0:
            part_tp[0, k] = partial
            stat_tp[0, k] = tile
            return
        part_send[j, k] = partial
        stat_send[j, k] = tile
        target = {"tp": tp_from(j)}
        copies[j, k] = (
            remote(
                stat_send.at[j, k],
                stat_tp.at[j, k],
                st_send.at[j, k],
                st_recv.at[j, k],
                target,
            ),
            remote(
                part_send.at[j, k],
                part_tp.at[j, k],
                pt_send.at[j, k],
                pt_recv.at[j, k],
                target,
            ),
        )

    for k in range(kv_local):
        attend(0, k)
    arrived = set()
    for k in range(kv_local):
        for j in far_first if k == kv_local - 1 else range(1, nt):
            if j not in arrived and relayed(j + 1):
                arrived.add(j)
                relay(j)
            elif j not in arrived:
                arrived.add(j)
                with jax.named_scope(f"q_tp_wait{j}"):
                    for a in range(nz):
                        q_from_tp[a, j].wait_recv()
            attend(j, k)

    def columns_of(pieces):
        height = -(-len(pieces) // 8) * 8
        index = lax.broadcasted_iota(jnp.int32, (height, rows), 0)
        tile = jnp.zeros((height, rows), jnp.float32)
        for i, piece in enumerate(pieces):
            tile = jnp.where(index == i, piece, tile)
        return tile.T

    from_z = {}
    for k in range(kv_local):
        with jax.named_scope(f"part_wait{k}"):
            for j in range(1, nt):
                for copy in copies[j, k]:
                    copy.wait_recv()
        peaks = [stat_tp[j, k, 0:1, :] for j in range(nt)]
        top = peaks[0]
        for piece in peaks[1:]:
            top = jnp.maximum(top, piece)
        scale = [jnp.exp2(piece - top) for piece in peaks]
        total = scale[0] * stat_tp[0, k, 1:2, :]
        for j in range(1, nt):
            total += scale[j] * stat_tp[j, k, 1:2, :]
        spread_scale = columns_of(scale)
        joined = spread_scale[:, 0:1] * part_tp[0, k].astype(jnp.float32)
        for j in range(1, nt):
            joined += spread_scale[:, j : j + 1] * part_tp[j, k].astype(jnp.float32)
        joined = joined.astype(jnp.bfloat16)
        index = lax.broadcasted_iota(jnp.int32, (8, rows), 0)
        tile = jnp.where(index == 0, top, total)
        z_stat_send[k] = tile
        z_stat[0, k] = tile
        z_part[0, k] = joined[:sub]
        for a in range(1, nz):
            z_send[a, k] = joined[a * sub : (a + 1) * sub]
        for a in reversed(z_order):
            target = {"kvb": z_back(a)}
            from_z[a, k] = (
                remote(
                    z_stat_send.at[k],
                    z_stat.at[a, k],
                    zs_send.at[a, k],
                    zs_recv.at[a, k],
                    target,
                ),
                remote(
                    z_send.at[a, k],
                    z_part.at[a, k],
                    zp_send.at[a, k],
                    zp_recv.at[a, k],
                    target,
                ),
            )

    step = width
    reduced = {}
    for k in range(kv_local):
        with jax.named_scope(f"z_wait{k}"):
            for a in z_order:
                for copy in from_z[a, k]:
                    copy.wait_recv()
        spread_stat = columns_of([z_stat[a, k, i : i + 1, :] for a in range(nz) for i in range(2)])
        peaks = [spread_stat[a * sub : (a + 1) * sub, 2 * a : 2 * a + 1] for a in range(nz)]
        sums = [spread_stat[a * sub : (a + 1) * sub, 2 * a + 1 : 2 * a + 2] for a in range(nz)]
        top = fresh[k]
        for piece in peaks:
            top = jnp.maximum(top, piece)
        denominator = jnp.exp2(fresh[k] - top)
        numerator = denominator * new_buf[k, 1]
        for a in range(nz):
            scale = jnp.exp2(peaks[a] - top)
            denominator += scale * sums[a]
            numerator += scale * z_part[a, k].astype(jnp.float32)
        row_buf[k] = numerator / denominator
        for q in range(per_kv):
            lhs_buf[k, 0:seq_rep, q * HD : (q + 1) * HD] = row_buf[
                k, q * seq_rep : (q + 1) * seq_rep, :
            ]
        attended = lhs_buf[k].astype(jnp.bfloat16)
        with jax.named_scope(f"weight_wait{k}"):
            for copy in weight_copies[k * pieces : (k + 1) * pieces]:
                copy.wait()
        for j in far_first + [0]:
            column = tp_to(j) * width

            def column_step(i, carry, j=j, k=k, column=column, attended=attended):
                at = pl.ds(pl.multiple_of(i * step, LANES), step)
                source = pl.ds(pl.multiple_of(column + i * step, LANES), step)
                got = jnp.dot(
                    attended,
                    weight_buf[k * depth : (k + 1) * depth, source],
                    preferred_element_type=jnp.float32,
                )[:seq_rep]
                if k > 0:
                    got += proj_sum[j, :, at]
                if j > 0 and k == kv_local - 1:
                    proj_send[j, :, at] = got.astype(jnp.bfloat16)
                else:
                    proj_sum[j, :, at] = got
                return carry

            lax.fori_loop(0, width // step, column_step, 0)
            if j > 0 and k == kv_local - 1:
                reduced[j] = remote(
                    proj_send.at[j],
                    proj_recv.at[j],
                    rs_send.at[j],
                    rs_recv.at[j],
                    {"tp": tp_to(j)},
                )
    summed = proj_sum[0]
    with jax.named_scope("sum_wait"):
        for j in far_first:
            reduced[j].wait_recv()
    for j in far_first:
        summed += proj_recv[j].astype(jnp.float32)
    stream = (residual_ref[...].astype(jnp.float32) + summed).astype(jnp.bfloat16)
    stream_wide = stream.astype(jnp.float32)
    stream_ref[...] = stream_wide
    square = jnp.sum(stream_wide * stream_wide, axis=1, keepdims=True)
    ss_send[...] = jnp.broadcast_to(square, ss_send.shape)
    squares = [
        remote(ss_send, ss_recv.at[j], sq_send.at[j], sq_recv.at[j], {"tp": tp_to(j)})
        for j in far_first
    ]
    gain = gain_ref[...].astype(jnp.float32).reshape(1, width)
    with jax.named_scope("square_wait"):
        for copy in squares:
            copy.wait_recv()
    for j in range(1, nt):
        square += ss_recv[j][:, 0:1]
    mean_square = square * (1.0 / (width * nt))
    factor_ref[...] = lax.rsqrt(mean_square + EPSILON) * gain
    for copy in pending:
        copy.wait_send()


def on_device(
    residual,
    queries,
    new_kv,
    kv_cache,
    lengths,
    slot_seq,
    slot_block,
    block_counts,
    out_weight,
    norm_gain,
):
    nt = lax.axis_size("tp")
    nz = lax.axis_size("kvb")
    seq_rep = residual.shape[0]
    local_heads = queries.shape[1] // HD
    kv_local = max(1, local_heads // GROUP_HEADS)
    sub = local_heads // kv_local * seq_rep
    rows = nz * sub
    slots = kv_cache.shape[0]
    tokens = slots * BLK
    width = norm_gain.shape[0]
    depth = out_weight.shape[0]
    bf16, f32 = jnp.bfloat16, jnp.float32
    dma = pltpu.SemaphoreType.DMA
    vmem = pl.BlockSpec(memory_space=pltpu.VMEM)
    smem = pl.BlockSpec(memory_space=pltpu.SMEM)
    hbm = pl.BlockSpec(memory_space=pl.ANY)

    def body(*refs):
        kernel(nz, nt, seq_rep, local_heads, *refs)

    stream, factor = pl.pallas_call(
        body,
        out_shape=(
            jax.ShapeDtypeStruct((seq_rep, width), f32),
            jax.ShapeDtypeStruct((seq_rep, width), f32),
        ),
        in_specs=[smem, smem] + [hbm] * 8,
        out_specs=(vmem, vmem),
        scratch_shapes=[
            pltpu.VMEM((1, slots), jnp.int32),
            pltpu.VMEM((1, slots), jnp.int32),
            pltpu.VMEM((seq_rep, width), bf16),
            pltpu.VMEM(queries.shape, bf16),
            pltpu.VMEM(new_kv.shape, bf16),
            pltpu.VMEM((width,), bf16),
            pltpu.VMEM((tokens, kv_cache.shape[2]), bf16),
            pltpu.VMEM(out_weight.shape, bf16),
            pltpu.VMEM((rows, tokens), f32),
            pltpu.VMEM((kv_local, sub, HD), f32),
            pltpu.VMEM((kv_local, 2, sub, HD), f32),
            pltpu.VMEM((nt, nz, kv_local, sub, HD), bf16),
            pltpu.VMEM((nt, kv_local, rows, HD), bf16),
            pltpu.VMEM((nt, kv_local, 8, rows), f32),
            pltpu.VMEM((nt, kv_local, rows, HD), bf16),
            pltpu.VMEM((nt, kv_local, 8, rows), f32),
            pltpu.VMEM((nz, kv_local, sub, HD), bf16),
            pltpu.VMEM((kv_local, 8, rows), f32),
            pltpu.VMEM((nz, kv_local, sub, HD), bf16),
            pltpu.VMEM((nz, kv_local, 8, rows), f32),
            pltpu.VMEM((kv_local, 16, depth // kv_local), f32),
            pltpu.VMEM((nt, seq_rep, width), f32),
            pltpu.VMEM((nt, seq_rep, width), bf16),
            pltpu.VMEM((nt, seq_rep, width), bf16),
            pltpu.VMEM((seq_rep, LANES), f32),
            pltpu.VMEM((nt, seq_rep, LANES), f32),
            dma((6,)),
            dma,
            dma((kv_local * 4,)),
            dma((nz,)),
            dma((nz,)),
            dma((nz, nt)),
            dma((nz, nt)),
            dma((nt, kv_local)),
            dma((nt, kv_local)),
            dma((nt, kv_local)),
            dma((nt, kv_local)),
            dma((nz, kv_local)),
            dma((nz, kv_local)),
            dma((nz, kv_local)),
            dma((nz, kv_local)),
            dma((nt,)),
            dma((nt,)),
            dma((nt,)),
            dma((nt,)),
        ],
        compiler_params=pltpu.CompilerParams(
            collective_id=0, has_side_effects=True, vmem_limit_bytes=62 * 1024 * 1024
        ),
    )(
        lengths,
        block_counts,
        slot_seq.reshape(1, slots),
        slot_block.reshape(1, slots),
        residual,
        queries,
        new_kv,
        norm_gain,
        kv_cache.reshape(tokens, kv_cache.shape[2]),
        out_weight,
    )
    return (stream.astype(bf16), (stream * factor).astype(bf16))


def solution(mesh):
    placed = (
        P(("groups", "kvb"), None),
        P(("groups", "kvb"), "tp"),
        P(("groups", "kvb"), None),
        P(("groups", "kvb", "tp"), None, None),
        P("groups"),
        P(("groups", "kvb", "tp")),
        P(("groups", "kvb", "tp")),
        P(("groups", "kvb", "tp")),
        P("tp", None),
        P("tp"),
    )
    return jax.shard_map(
        on_device,
        mesh=mesh,
        in_specs=placed,
        out_specs=(P(("groups", "kvb"), "tp"), P(("groups", "kvb"), "tp")),
        check_vma=False,
    )
```
